32 devices in a mesh: order: 8 (over y, x, core), axial: 4 (over z).
Axes of the slice: x: 2, y: 2, z: 4, core: 2. Of those that a mesh axis runs over, the one named last changes fastest.
Arguments:
- coefficients: bfloat16 [4, 2, 1024, 8, 1024], P(None, None, 'order', 'axial'), may hold values from -0.005859375 to 0.005859375
- order_lists: int32 [1024], replicated, may hold values from 0 to 1023, as said below
- lengths: int32 [1024], replicated, may hold values from 128 to 1024, as said below
Outputs:
- advection: bfloat16 [3, 2, 1024, 8, 1024], P(None, None, 'order', 'axial')
The draws below stay inside these ranges and needn't reach their ends.
Inputs may be any that keep to these rules, and one draw needn't show every extreme that they name: `order_lists`: a permutation of the orders 0 to 1023; the device with index j along order holds slots j * 128 to (j + 1) * 128 - 1 of coefficients and advection. lengths[m] minus (128 + ((1023 - m) * 768) // 1023) lies in 0 to 128.
All inputs are finite; a program needn't handle non-finite values.
Results may differ from the reference program's by a relative error of at most 0.0095.
Values may be sent and summed in bfloat16 or wider, within the bound.
A program may use at most 128 MiB of HBM per device.

```python
import math
import jax
import jax.numpy as jnp
from jax import lax

M = 1024
R = 1024
K = 1024
NA = 2048
NZ = 8
MO = 128


def draw_order_lists(key, part):
    key_spread, key_blocks, key_shuffle = jax.random.split(jax.random.fold_in(key, 11), 3)
    group_count = M // MO
    position = jnp.arange(M, dtype=jnp.int32)
    spread = jax.random.randint(key_spread, (M,), 0, 4 * MO, dtype=jnp.int32)
    dealt_ids = jnp.argsort((position + spread) * M + position, stable=True).astype(jnp.int32)
    blocks = dealt_ids.reshape(group_count, MO)
    blocks = jnp.take(blocks, jax.random.permutation(key_blocks, group_count), axis=0)
    shuffle = jax.random.randint(key_shuffle, (group_count, MO), 0, M, dtype=jnp.int32)
    inside = jnp.argsort(shuffle * MO + jnp.arange(MO, dtype=jnp.int32)[None, :], axis=1, stable=True)
    blocks = jnp.take_along_axis(blocks, inside, axis=1)
    return blocks.reshape(M).astype(jnp.int32)


def draw_lengths(key, part):
    position = jnp.arange(M, dtype=jnp.int32)
    jitter = jax.random.randint(jax.random.fold_in(key, 23), (M,), 0, K // 8 + 1, dtype=jnp.int32)
    jitter = jnp.where(position == 0, K // 8, jnp.where(position == M - 1, 0, jitter))
    trend = K // 8 + (M - 1 - position) * (K - K // 4) // (M - 1)
    return (trend + jitter).astype(jnp.int32)


def steps_of(key, extent, shards, least, largest):
    def one(dim, parts):
        heights = jax.random.uniform(jax.random.fold_in(jax.random.fold_in(key, 6), dim), (parts,), jnp.float32, least / len(shards), largest / len(shards))
        return jnp.repeat(jnp.exp(heights), extent[dim] // parts).reshape((-1,) + (1,) * (len(extent) - dim - 1))

    loudness = one(*shards[0])
    for cut in shards[1:]:
        loudness = loudness * one(*cut)
    return loudness


def normal_values(key, shape, deviation, bound, cuts=(), kind=jnp.bfloat16):
    drawn = deviation * jax.random.normal(key, shape, jnp.float32)
    if cuts:
        drawn = drawn * steps_of(key, shape, cuts, -0.22, 0.18)
    return jnp.clip(drawn, -bound, bound).astype(kind)


def setup_inputs(seed: int = 0) -> dict:
    key_list = jax.random.split(jax.random.key(seed), 4)
    return {
        "coefficients": normal_values(key_list[0], (4, 2, M, NZ, K), (M * K) ** -0.5, 0.005859375, ((2, 8), (3, 4))),
        "order_lists": draw_order_lists(jax.random.fold_in(key_list[3], 71), 0),
        "lengths": draw_lengths(jax.random.fold_in(key_list[3], 71), 0),
    }


def radial_tables(radius_count, mode_count):
    radius_ids = jnp.arange(radius_count, dtype=jnp.int32)
    mode_ids = jnp.arange(mode_count, dtype=jnp.int32)
    phases = mode_ids[None, :] * (2 * radius_ids[:, None] + 1) % (4 * radius_count)
    angles_rad = phases.astype(jnp.float32) * (math.pi / (2 * radius_count))
    synthesis = jnp.cos(angles_rad).astype(jnp.bfloat16)
    analysis = (jnp.cos(angles_rad.T) * math.sqrt(2.0 / radius_count)).astype(jnp.bfloat16)
    return (synthesis, analysis)

def azimuthal_tables(order_ids, point_count):
    points = jnp.arange(point_count, dtype=jnp.int32)
    phases = order_ids[..., None] * points % point_count
    angles_rad = phases.astype(jnp.float32) * (2.0 * math.pi / point_count)
    cosines = jnp.cos(angles_rad)
    sines = jnp.sin(angles_rad)
    weight = jnp.where(order_ids == 0, 1.0, 2.0).astype(jnp.float32)[..., None]
    forward = jnp.stack((weight * cosines, -weight * sines), axis=-3).astype(jnp.bfloat16)
    factor = math.sqrt(2.0 / point_count)
    inverse = jnp.stack((cosines * factor, -sines * factor), axis=-3).astype(jnp.bfloat16)
    return (forward, inverse)

def reference(coefficients, order_lists, lengths):
    synthesis, analysis = radial_tables(R, K)
    forward, inverse = azimuthal_tables(order_lists, NA)
    synthesis_f = synthesis.astype(jnp.float32)
    analysis_f = analysis.astype(jnp.float32)
    forward_f = forward.astype(jnp.float32)
    inverse_f = inverse.astype(jnp.float32)
    slot_lengths = jnp.take(lengths, order_lists.astype(jnp.int32))
    retained = jnp.arange(K, dtype=jnp.int32)[None, :] < slot_lengths[:, None]
    plane_major = jnp.moveaxis(coefficients, 3, 0)

    def to_physical(plane_in):
        masked = jnp.where(retained[None, None], plane_in, 0).astype(jnp.float32)
        radial = jnp.einsum('fcmk,rk->fcmr', masked, synthesis_f).astype(jnp.bfloat16)
        physical = jnp.einsum('fcmr,cmj->frj', radial.astype(jnp.float32), forward_f)
        return physical.astype(jnp.bfloat16)
    physical = lax.map(to_physical, plane_major)
    plane_total = physical.shape[0]

    def advect(position):

        def plane_at(offset):
            where_at = ((position + offset) % plane_total).astype(jnp.int32)
            return lax.dynamic_index_in_dim(physical, where_at, 0, keepdims=False).astype(jnp.float32)
        current = plane_at(0)
        ahead_one = plane_at(1)
        behind_one = plane_at(-1)
        ahead_two = plane_at(2)
        behind_two = plane_at(-2)
        gradient = (8.0 * (ahead_one[:3] - behind_one[:3]) - (ahead_two[:3] - behind_two[:3])) / 12.0
        products = (current[3][None] * gradient).astype(jnp.bfloat16)
        spectral = jnp.einsum('grj,cmj->gcmr', products.astype(jnp.float32), inverse_f).astype(jnp.bfloat16)
        result = jnp.einsum('gcmr,kr->gcmk', spectral.astype(jnp.float32), analysis_f)
        return jnp.where(retained[None, None], result, 0.0).astype(jnp.bfloat16)
    advected = lax.map(advect, jnp.arange(plane_total, dtype=jnp.int32))
    return jnp.moveaxis(advected, 0, 3)
```

```python
import functools
import math

import jax
import jax.numpy as jnp
from jax import lax
from jax.experimental import pallas as pl
from jax.experimental.pallas import tpu as pltpu
from jax.sharding import PartitionSpec as P

R = 1024
LANES = 128
HALO = 2
MESH = pl.DeviceIdType.MESH


def cosine(phase, period):
    turn = jnp.abs((phase & (period - 1)) - period // 2) - period // 4
    y = turn.astype(jnp.float32) * (2.0 * math.pi / period)
    y2 = y * y
    total = jnp.full_like(y, -1.0 / 39916800.0)
    for term in (1.0 / 362880.0, -1.0 / 5040.0, 1.0 / 120.0, -1.0 / 6.0, 1.0):
        total = total * y2 + term
    return total * y


def fill_waves(ids, period, columns, store):
    lane = lax.broadcasted_iota(jnp.int32, ids.shape, 1)
    base, step = ids * lane, ids * LANES
    quarter = period // 4
    c, s = cosine(base, period), cosine(base - quarter, period)
    cs, ss = cosine(step, period), cosine(step - quarter, period)
    for h in range(columns // LANES):
        store(h, c, s)
        c, s = c * cs - s * ss, s * cs + c * ss


def stencil(at, z):
    return (8.0 * (at(z + 3) - at(z + 1)) - (at(z + 4) - at(z))) / 12.0


def dot(a, b, dims):
    return lax.dot_general(a, b, (dims, ((), ())), preferred_element_type=jnp.float32)


def advect_kernel(
    chunks, xs, kept, ids, out,
    synthesis, table, send, recv, phys, halo_a, halo_p, grad, prod, back, home,
    fs_sem, fr_sem, bs_sem, br_sem, zs_sem, zr_sem, as_sem, ar_sem,
):
    n = lax.axis_size("order")
    nz = lax.axis_size("axial")
    me = lax.axis_index("order")
    za = lax.axis_index("axial")
    after, before = lax.rem(za + 1, nz), lax.rem(za + nz - 1, nz)
    _, planes, part, modes = xs.shape
    slots = part // 2
    band = synthesis.shape[0] // n
    points = table.shape[1]
    radii = synthesis.shape[0]
    factor = math.sqrt(2.0 / points)

    barrier = pltpu.get_barrier_semaphore()

    def greet(d, _):
        peer = lax.rem(me + 1 + d, n)
        pl.semaphore_signal(barrier, inc=1, device_id={"order": peer}, device_id_type=MESH)
        return 0

    lax.fori_loop(0, n - 1, greet, 0)
    for peer in (after, before):
        pl.semaphore_signal(barrier, inc=1, device_id={"axial": peer}, device_id_type=MESH)
    pl.semaphore_wait(barrier, n + 1)

    def z_copy(source, target, s_sem, r_sem, peer):
        return pltpu.make_async_remote_copy(
            src_ref=source, dst_ref=target, send_sem=s_sem, recv_sem=r_sem,
            device_id={"axial": peer}, device_id_type=MESH,
        )

    def a_copy(side):
        source = xs.at[0, pl.ds(planes - HALO if side == 0 else 0, HALO)]
        peer = after if side == 0 else before
        return z_copy(source, halo_a.at[side], as_sem.at[side], ar_sem.at[side], peer)

    def p_copy(f, side, q):
        rows = band // chunks
        source = phys.at[f, pl.ds(planes - HALO if side == 0 else 0, HALO), pl.ds(q * rows, rows)]
        target = halo_p.at[f - 1, side, :, pl.ds(q * rows, rows)]
        peer = after if side == 0 else before
        return z_copy(source, target, zs_sem.at[f - 1, side, q], zr_sem.at[f - 1, side, q], peer)

    for side in range(2):
        a_copy(side).start()

    tall = min(32, slots, band)

    def synthesis_rows(b, _):
        first = pl.multiple_of(b * tall, tall)
        row = lax.broadcasted_iota(jnp.int32, (tall, LANES), 0) + first

        def store(h, c, s):
            synthesis[pl.ds(first, tall), h * LANES : (h + 1) * LANES] = c.astype(jnp.bfloat16)

        fill_waves(2 * row + 1, 4 * radii, modes, store)
        return 0

    lax.fori_loop(0, radii // tall, synthesis_rows, 0)

    def f_copy(f, d):
        peer = lax.rem(me + 1 + d, n)
        return pltpu.make_async_remote_copy(
            src_ref=send.at[f, peer], dst_ref=recv.at[f, me],
            send_sem=fs_sem.at[f, d], recv_sem=fr_sem.at[f, d],
            device_id={"order": peer}, device_id_type=MESH,
        )

    def forward(f, source):
        def body(d, _):
            peer = lax.rem(me + 1 + d, n)
            rows = pl.multiple_of(peer * band, band)
            for z in range(planes):
                send[f, peer, z * band : (z + 1) * band, :] = dot(
                    synthesis[pl.ds(rows, band), :], source(z), ((1,), (1,))
                ).astype(jnp.bfloat16)

            @pl.when(d < n - 1)
            def _():
                f_copy(f, d).start()

            return 0

        lax.fori_loop(0, n, body, 0)
        recv[f, me] = send[f, me]

    def forward_wait(f):
        def body(d, _):
            f_copy(f, d).wait_recv()
            return 0

        lax.fori_loop(0, n - 1, body, 0)

    for f in (1, 3, 2):
        forward(f, lambda z: xs[f, z])

    def table_rows(b, _):
        first = pl.multiple_of(b * tall, tall)
        group = first // slots
        place = pl.multiple_of(group * part + (first - group * slots), tall)

        def store(h, c, s):
            cols = slice(h * LANES, (h + 1) * LANES)
            table[pl.ds(place, tall), cols] = c.astype(jnp.bfloat16)
            table[pl.ds(place + slots, tall), cols] = (-s).astype(jnp.bfloat16)

        fill_waves(ids[pl.ds(first, tall), :], points, points, store)
        return 0

    lax.fori_loop(0, n * slots // tall, table_rows, 0)

    wide = min(512, points)

    def around(f, use):
        def body(t, _):
            cols = pl.ds(pl.multiple_of(t * wide, wide), wide)
            total = dot(recv[f, 0], table[0:part, cols], ((1,), (0,)))
            for i in range(1, n):
                total += dot(recv[f, i], table[i * part : (i + 1) * part, cols], ((1,), (0,)))
            use(cols, total)
            return 0

        lax.fori_loop(0, points // wide, body, 0)

    def physical(f):
        def use(cols, total):
            for z in range(planes):
                phys[f, z, :, cols] = total[z * band : (z + 1) * band].astype(jnp.bfloat16)

        forward_wait(f)
        around(f, use)

    physical(1)
    for q in range(chunks):
        for side in range(2):
            p_copy(1, side, q).start()
    physical(3)
    physical(2)
    for q in range(chunks):
        for side in range(2):
            p_copy(2, side, q).start()

    def b_copy(g, q, count, d):
        rows = band // count
        peer = lax.rem(me + 1 + d, n)
        return pltpu.make_async_remote_copy(
            src_ref=back.at[g, peer, :, pl.ds(q * rows, rows)],
            dst_ref=home.at[g, :, pl.ds(me * band + q * rows, rows)],
            send_sem=bs_sem.at[g, q, d], recv_sem=br_sem.at[g, q, d],
            device_id={"order": peer}, device_id_type=MESH,
        )

    def inverse(g, q, count):
        rows = band // count
        values = prod.at[0 : planes * rows]

        def body(d, _):
            peer = lax.rem(me + 1 + d, n)
            first = pl.multiple_of(peer * part, part)
            term = dot(values[...], table[pl.ds(first, part), :], ((1,), (1,))) * factor
            for z in range(planes):
                back[g, peer, z, q * rows : (q + 1) * rows, :] = term[
                    z * rows : (z + 1) * rows
                ].astype(jnp.bfloat16)

            @pl.when(d < n - 1)
            def _():
                b_copy(g, q, count, d).start()

            return 0

        lax.fori_loop(0, n, body, 0)
        place = pl.multiple_of(me * band + q * rows, rows)
        for z in range(planes):
            home[g, z, pl.ds(place, rows), :] = back[g, me, z, q * rows : (q + 1) * rows, :]

    def analysis(g, count):
        for q in range(count):
            def body(d, _):
                b_copy(g, q, count, d).wait_recv()
                return 0

            lax.fori_loop(0, n - 1, body, 0)
        for z in range(planes):
            for k in range(0, modes, wide):
                term = dot(home[g, z], synthesis[:, k : k + wide], ((0,), (0,)))
                for c in range(2):
                    out[g, z, c, :, k : k + wide] = (
                        term[c * slots : (c + 1) * slots] * kept[:, k : k + wide]
                    ).astype(out.dtype)

    for side in range(2):
        a_copy(side).wait_recv()

    def plane(z):
        if z < HALO:
            return halo_a.at[0, z]
        if z < HALO + planes:
            return xs.at[0, z - HALO]
        return halo_a.at[1, z - HALO - planes]

    def stencil_rows(b, _):
        rows = pl.ds(pl.multiple_of(b * tall, tall), tall)
        for z in range(planes):
            grad[z, rows, :] = stencil(
                lambda p: plane(p)[rows, :].astype(jnp.float32), z
            ).astype(jnp.bfloat16)
        return 0

    lax.fori_loop(0, part // tall, stencil_rows, 0)
    forward(0, lambda z: grad[z])
    forward_wait(0)

    def multiply(cols, total):
        for z in range(planes):
            rows = slice(z * band, (z + 1) * band)
            prod[rows, cols] = (phys[3, z, :, cols].astype(jnp.float32) * total[rows]).astype(
                jnp.bfloat16
            )

    around(0, multiply)
    inverse(0, 0, 1)

    def advance(g, q):
        rows = band // chunks
        for side in range(2):
            p_copy(g, side, q).wait_recv()

        def level(z):
            if z < HALO:
                return halo_p.at[g - 1, 0, z]
            if z < HALO + planes:
                return phys.at[g, z - HALO]
            return halo_p.at[g - 1, 1, z - HALO - planes]

        def body(t, _):
            cols = pl.ds(pl.multiple_of(t * wide, wide), wide)
            here = slice(q * rows, (q + 1) * rows)
            for z in range(planes):
                slope = stencil(lambda p: level(p)[here, cols].astype(jnp.float32), z)
                prod[z * rows : (z + 1) * rows, cols] = (
                    phys[3, z, here, cols].astype(jnp.float32) * slope
                ).astype(jnp.bfloat16)
            return 0

        lax.fori_loop(0, points // wide, body, 0)
        inverse(g, q, chunks)

    advance(1, 0)
    analysis(0, 1)
    for q in range(1, chunks):
        advance(1, q)
    advance(2, 0)
    analysis(1, chunks)
    for q in range(1, chunks):
        advance(2, q)
    analysis(2, chunks)

    for side in range(2):
        a_copy(side).wait_send()
        for f in (1, 2):
            for q in range(chunks):
                p_copy(f, side, q).wait_send()

    def drain(d, _):
        for f in range(4):
            f_copy(f, d).wait_send()
        b_copy(0, 0, 1, d).wait_send()
        for g in (1, 2):
            for q in range(chunks):
                b_copy(g, q, chunks, d).wait_send()
        return 0

    lax.fori_loop(0, n - 1, drain, 0)


def call_advect(xs, kept, ids, points):
    fields, planes, part, modes = xs.shape
    n = lax.axis_size("order")
    band = R // n
    slots = part // 2
    chunks = max(1, min(4, band // 32))
    held = pl.BlockSpec(memory_space=pltpu.VMEM)
    half = jnp.bfloat16
    dma = pltpu.SemaphoreType.DMA
    return pl.pallas_call(
        functools.partial(advect_kernel, chunks),
        in_specs=[held] * 3,
        out_specs=held,
        out_shape=jax.ShapeDtypeStruct((3, planes, 2, slots, modes), half),
        scratch_shapes=[
            pltpu.VMEM((R, modes), half),
            pltpu.VMEM((n * part, points), half),
            pltpu.VMEM((fields, n, planes * band, part), half),
            pltpu.VMEM((fields, n, planes * band, part), half),
            pltpu.VMEM((fields, planes, band, points), half),
            pltpu.VMEM((2, HALO, part, modes), half),
            pltpu.VMEM((2, 2, HALO, band, points), half),
            pltpu.VMEM((planes, part, modes), half),
            pltpu.VMEM((planes * band, points), half),
            pltpu.VMEM((3, n, planes, band, part), half),
            pltpu.VMEM((3, planes, R, part), half),
            dma((fields, n - 1)),
            dma((fields, n - 1)),
            dma((3, chunks, n - 1)),
            dma((3, chunks, n - 1)),
            dma((2, 2, chunks)),
            dma((2, 2, chunks)),
            dma((2,)),
            dma((2,)),
        ],
        compiler_params=pltpu.CompilerParams(
            collective_id=0, has_side_effects=True, vmem_limit_bytes=66_000_000
        ),
        name="advect",
    )(xs, kept, ids)


def shards(coefficients, order_lists, lengths):
    fields, parts, slots, planes, modes = coefficients.shape
    orders = order_lists.shape[0]
    points = 2 * orders
    owned = lax.dynamic_slice_in_dim(order_lists, lax.axis_index("order") * slots, slots)
    catalog = jnp.arange(orders, dtype=jnp.int32)
    own_lengths = jnp.sum(
        jnp.where(owned[:, None] == catalog[None, :], lengths[None, :], 0), axis=1
    )
    retained = jnp.arange(modes, dtype=jnp.int32)[None, :] < own_lengths[:, None]
    weight = jnp.where(owned == 0, 1.0, 2.0)[:, None]
    scale = jnp.where(retained, weight, 0.0).astype(coefficients.dtype)
    kept = jnp.where(retained, math.sqrt(2.0 / R), 0.0).astype(jnp.float32)
    xs = jnp.transpose(coefficients, (0, 3, 1, 2, 4)) * scale
    xs = xs.reshape(fields, planes, parts * slots, modes)
    ids = jnp.broadcast_to(order_lists[:, None], (orders, LANES))
    result = call_advect(xs, kept, ids, points)
    return jnp.transpose(result, (0, 2, 3, 1, 4))


def solution(mesh):
    placed = (P(None, None, "order", "axial", None), P(), P())
    return jax.shard_map(
        shards,
        mesh=mesh,
        in_specs=placed,
        out_specs=P(None, None, "order", "axial", None),
        check_vma=False,
    )
```
